32 devices in a mesh: dom: 16 (over z, y, x), feat: 2 (over core).
Axes of the slice: x: 2, y: 2, z: 4, core: 2. Of those that a mesh axis runs over, the one named last changes fastest.
Arguments:
- features: bfloat16 [32768, 608], P('dom', 'feat'), may hold values from -6 to 6
- weight: bfloat16 [608, 256], replicated, may hold values from -0.25 to 0.25
- out_bias: float32 [256], P('feat'), may hold values from -3 to 3
- tile_values: bfloat16 [1728, 128, 128], P('dom'), may hold values from -0.25 to 0.25
- tile_rows: int32 [1728], P('dom'), may hold values from 0 to 15
- tile_cols: int32 [1728], P('dom'), may hold values from 0 to 81, as said below
- tile_count: int32 [16], P('dom'), may hold values from 10 to 108, as said below
- send_rows: int32 [16, 8, 1024], P('dom'), may hold values from 0 to 2047
- hub_ids: int32 [256], replicated, may hold values from 0 to 32767, as said below
Outputs:
- activations: bfloat16 [32768, 256], P('dom', 'feat')
The draws below stay inside these ranges and needn't reach their ends.
Inputs may be any that keep to these rules, and one draw needn't show every extreme that they name: `tile_count`: slots at or past a partition's count are not part of the graph; some partition uses all 108 slots. `tile_cols`: column blocks index the extended row space of the slot's partition. `hub_ids`: distinct vertex ids; vertex v belongs to partition v // 2048; no partition owns more than 48 hubs, and some partition owns exactly 48.
All inputs are finite; a program needn't handle non-finite values.
Results may differ from the reference program's by a relative error of at most 0.0044.
Values may be sent and summed in bfloat16 or wider, within the bound.
A program may use at most 64 MiB of HBM per device.

```python
import jax
import jax.numpy as jnp
from jax import lax

F_IN = 608
HID = 256
BLK = 128
VDEV = 2048
REACH = 4
HUB_MOST = 48
TILE_MOST = 108
HALO = 1024
HUBS = 256
EXT = 10496
VERTICES = 32768
PARTITIONS = 16
TILES = 1728
N_DOM = 16


def draw_tile_count(key, part):
    lowest = 2 * REACH + 2
    spread = TILE_MOST - lowest + 1
    key_list = jax.random.split(jax.random.fold_in(key, 11), 2)
    raw_draws = jax.random.randint(key_list[0], (N_DOM,), 0, spread)
    counts = lowest + raw_draws * raw_draws // spread
    fullest = jax.random.randint(key_list[1], (), 0, N_DOM)
    counts = jnp.where(jnp.arange(N_DOM) == fullest, TILE_MOST, counts)
    return counts.astype(jnp.int32)


def draw_tile_cols(key, part):
    block_total = ((1 + REACH) * VDEV + HUBS) // BLK
    hub_first = (1 + REACH) * VDEV // BLK
    key_list = jax.random.split(jax.random.fold_in(key, 23), 3)
    columns = jax.random.randint(key_list[0], (N_DOM, TILE_MOST), 0, block_total)
    position = jnp.arange(TILE_MOST)[None, :]
    segment_start = (VDEV + position * (VDEV // 2)) // BLK
    hub_pick = jax.random.randint(key_list[1], (N_DOM, 1), hub_first, block_total)
    local_pick = jax.random.randint(key_list[2], (N_DOM, 1), 0, VDEV // BLK)
    columns = jnp.where(position < 2 * REACH, segment_start, columns)
    columns = jnp.where(position == 2 * REACH, hub_pick, columns)
    columns = jnp.where(position == 2 * REACH + 1, local_pick, columns)
    return columns.reshape(N_DOM * TILE_MOST).astype(jnp.int32)


def draw_hub_ids(key, part):
    key_list = jax.random.split(jax.random.fold_in(key, 37), 4)
    slot_total = N_DOM * HUB_MOST
    positions = jnp.arange(slot_total)
    owners = positions // HUB_MOST
    ranks = positions % HUB_MOST
    device_level = jax.random.randint(key_list[0], (N_DOM,), 0, 4)
    fullest = jax.random.randint(key_list[1], (), 0, N_DOM)
    jitter = jax.random.randint(key_list[2], (slot_total,), 0, 1024)
    scores = (device_level[owners] * 1024 + jitter) * slot_total + positions
    scores = jnp.where(owners == fullest, scores + 8 * 1024 * slot_total, scores)
    chosen = jax.lax.top_k(scores.astype(jnp.int32), HUBS)[1]
    stride = VDEV // HUB_MOST
    shifts = jax.random.randint(key_list[3], (N_DOM,), 0, stride)
    chosen_owner = owners[chosen]
    local_rows = ranks[chosen] * stride + shifts[chosen_owner]
    return (chosen_owner * VDEV + local_rows).astype(jnp.int32)


def with_ends(drawn, own_key, smallest, largest):
    longest = drawn.shape.index(max(drawn.shape))
    spots = []
    for shift in (0, 1):
        where = [jax.random.randint(jax.random.fold_in(own_key, axis), (), 0, length) for axis, length in enumerate(drawn.shape)]
        where[longest] = (where[longest] + shift) % drawn.shape[longest]
        spots.append(tuple(where))
    return drawn.at[spots[0]].set(smallest).at[spots[1]].set(largest)


def block_levels(own_key, shape, cuts, low, top_value):
    level, own = 1.0, jax.random.fold_in(own_key, 6)
    for dim, blocks in cuts:
        draws = jnp.exp(jax.random.uniform(jax.random.fold_in(own, dim), (blocks,), jnp.float32, low / len(cuts), top_value / len(cuts)))
        level = level * jnp.repeat(draws, shape[dim] // blocks).reshape([-1 if axis == dim else 1 for axis in range(len(shape))])
    return level


def bell_draw(rng, extent, scale, bound, cuts=(), kind=jnp.bfloat16):
    values = jax.random.normal(rng, extent, jnp.float32) * scale
    if len(cuts) > 0:
        values = block_levels(rng, extent, cuts, -0.22, 0.18) * values
    return jnp.clip(values, min=-bound, max=bound).astype(kind)


def setup_inputs(seed: int = 0) -> dict:
    seeds = jax.random.split(jax.random.key(seed), 10)
    features = bell_draw(seeds[0], (VERTICES, F_IN), 1.0, 6.0, ((0, 16), (1, 2)))
    weight = bell_draw(seeds[1], (F_IN, HID), F_IN ** -0.5, 0.25)
    out_bias = bell_draw(seeds[2], (HID,), 0.5, 3.0, ((0, 2),), jnp.float32)
    tile_values = bell_draw(seeds[3], (TILES, BLK, BLK), (4 * BLK) ** -0.5, 0.25, ((0, 16),))
    tile_rows = with_ends(jax.random.randint(seeds[4], (TILES,), 0, VDEV // BLK), jax.random.fold_in(seeds[4], 1), 0, (VDEV // BLK) - 1).astype(jnp.int32)
    tile_cols = draw_tile_cols(jax.random.fold_in(seeds[9], 71), 0)
    tile_count = draw_tile_count(jax.random.fold_in(seeds[9], 71), 0)
    send_rows = with_ends(jax.random.randint(seeds[7], (PARTITIONS, 2 * REACH, HALO), 0, VDEV), jax.random.fold_in(seeds[7], 1), 0, VDEV - 1).astype(jnp.int32)
    hub_ids = draw_hub_ids(jax.random.fold_in(seeds[9], 71), 0)
    return {"features": features, "weight": weight, "out_bias": out_bias, "tile_values": tile_values, "tile_rows": tile_rows, "tile_cols": tile_cols, "tile_count": tile_count, "send_rows": send_rows, "hub_ids": hub_ids}


def reference(features, weight, out_bias, tile_values, tile_rows, tile_cols, tile_count, send_rows, hub_ids):
    projected = jnp.dot(features, weight, preferred_element_type=jnp.float32).astype(jnp.bfloat16)
    hub_rows = projected[hub_ids]
    offsets = jnp.array(list(range(-REACH, 0)) + list(range(1, REACH + 1)), jnp.int32)
    slot_ids = jnp.arange(2 * REACH).astype(jnp.int32)

    def one_partition(partition):
        own_rows = lax.dynamic_slice_in_dim(projected, partition * VDEV, VDEV, 0)
        sources = partition - offsets
        present = (sources >= 0) & (sources < N_DOM)
        clipped = jnp.clip(sources, 0, N_DOM - 1).astype(jnp.int32)
        listed = send_rows[clipped, slot_ids]
        picked = projected[clipped[:, None] * VDEV + listed]
        picked = jnp.where(present[:, None, None], picked, jnp.zeros_like(picked))
        extended = jnp.concatenate([own_rows, picked.reshape(REACH * VDEV, HID), hub_rows], 0)
        blocks = extended.reshape(EXT // BLK, BLK, HID)
        col_blocks = lax.dynamic_slice_in_dim(tile_cols, partition * TILE_MOST, TILE_MOST, 0)
        row_blocks = lax.dynamic_slice_in_dim(tile_rows, partition * TILE_MOST, TILE_MOST, 0)
        own_tiles = lax.dynamic_slice_in_dim(tile_values, partition * TILE_MOST, TILE_MOST, 0)
        products = jnp.einsum("tij,tjc->tic", own_tiles.astype(jnp.float32), blocks[col_blocks].astype(jnp.float32), precision=lax.Precision.HIGHEST)
        live_mask = jnp.arange(TILE_MOST).astype(jnp.int32) < tile_count[partition]
        products = jnp.where(live_mask[:, None, None], products, jnp.zeros_like(products))
        aggregate = jax.ops.segment_sum(products, row_blocks, num_segments=VDEV // BLK)
        return jnp.maximum(aggregate.reshape(VDEV, HID) + out_bias, 0.0).astype(jnp.bfloat16)

    result = lax.map(one_partition, jnp.arange(N_DOM, dtype=jnp.int32))
    return result.reshape(N_DOM * VDEV, HID)
```

```python
import functools
import math

import jax
import jax.numpy as jnp
from jax import lax
from jax.experimental import pallas as pl
from jax.experimental.pallas import tpu as pltpu
from jax.sharding import PartitionSpec as P

REACH = 4
HUB_MOST = 48


def passed_along(value, axis, steps):
    count = lax.axis_size(axis)
    initial, last = (max(0, -steps), min(count, count - steps))
    return lax.ppermute(value, axis, [(source, source + steps) for source in range(initial, last)])


def local_any(
    features, weight, out_bias, tile_values, tile_rows, tile_cols, tile_count, send_rows, hub_ids
):
    column_count = out_bias.shape[0]
    vertex_rows = features.shape[0]
    part_index = lax.axis_index("dom")
    feat_index = lax.axis_index("feat")
    weight_cols = lax.dynamic_slice_in_dim(weight, feat_index * column_count, column_count, 1)
    summed = jnp.dot(
        lax.all_gather(features, "feat", axis=1, tiled=True),
        weight_cols,
        preferred_element_type=jnp.float32,
    )
    projected = summed.astype(jnp.bfloat16)
    half_rows = send_rows.shape[2]
    slot_total = send_rows.shape[1]
    offsets = list(range(-REACH, 0)) + list(range(1, REACH + 1))
    packed_all = projected[send_rows[0].reshape(slot_total * half_rows)].reshape(
        slot_total, half_rows, column_count
    )
    received = []
    for slot_index, offset_value in enumerate(offsets):
        received.append(passed_along(packed_all[slot_index], "dom", offset_value))
    halo_block = jnp.concatenate(received, 0)
    owners = hub_ids // vertex_rows
    mine = owners == part_index
    local_index = jnp.clip(hub_ids - part_index * vertex_rows, 0, vertex_rows - 1)
    candidates = projected[local_index]
    hub_total = hub_ids.shape[0]
    positions = jnp.arange(hub_total, dtype=jnp.int32)
    earlier = (owners[:, None] == owners[None, :]) & (positions[:, None] > positions[None, :])
    ranks = jnp.sum(earlier.astype(jnp.int32), 1)
    selector = (
        mine[:, None] & (ranks[:, None] == jnp.arange(HUB_MOST, dtype=jnp.int32)[None, :])
    ).astype(jnp.bfloat16)
    slot_rows = lax.dot_general(
        selector, candidates, (((0,), (0,)), ((), ())), preferred_element_type=jnp.float32
    ).astype(jnp.bfloat16)
    gathered = lax.all_gather(slot_rows, "dom", axis=0, tiled=True)
    hub_block = gathered[owners * HUB_MOST + ranks]
    extended = jnp.concatenate([projected, halo_block, hub_block], 0)
    block_edge = tile_values.shape[1]
    blocks = extended.reshape(extended.shape[0] // block_edge, block_edge, column_count)
    products = jnp.einsum(
        "tij,tjc->tic", tile_values, blocks[tile_cols], preferred_element_type=jnp.float32
    )
    live_mask = jnp.arange(tile_values.shape[0], dtype=jnp.int32) < tile_count[0]
    block_count = vertex_rows // block_edge
    assignment = (
        (tile_rows[None, :] == jnp.arange(block_count, dtype=jnp.int32)[:, None])
        & live_mask[None, :]
    ).astype(jnp.float32)
    aggregate = jnp.einsum("rt,tic->ric", assignment, products, precision=lax.Precision.HIGHEST)
    activated = jnp.maximum(aggregate + out_bias[None, None, :], 0.0).astype(jnp.bfloat16)
    return activated.reshape(vertex_rows, column_count)

LANES = 128
GROUPS = 4
MESH = pl.DeviceIdType.MESH


def picked_rows(index, table_ref, groups):
    depth = table_ref.shape[0]
    group = index // depth
    within = index - group * depth
    positions = lax.broadcasted_iota(jnp.int32, (index.shape[0], depth), 1)
    chosen = (positions == within).astype(jnp.float32).astype(jnp.bfloat16)
    every = jnp.dot(chosen, table_ref[...], preferred_element_type=jnp.float32)
    width = table_ref.shape[1] // groups
    result = every[:, :width]
    for number in range(1, groups):
        part = every[:, number * width : (number + 1) * width]
        result = jnp.where(group == number, part, result)
    return result.astype(jnp.bfloat16)


def exchange_kernel(
    count, features_ref, weight_ref, send_ref, hub_ref, extended_ref,
    other_ref, total_ref, table_ref, index_ref, packed_ref, own_hubs_ref, hubs_ref,
    feature_sems, send_sems, receive_sems, hub_send_sems, hub_receive_sems,
):
    part = lax.axis_index("dom")
    feat = lax.axis_index("feat")
    vertex_rows, depth = features_ref.shape
    width = extended_ref.shape[1]
    slots, half_rows = send_ref.shape
    offsets = list(range(-REACH, 0)) + list(range(1, REACH + 1))
    hub_total = hub_ref.shape[1]
    halo_end = vertex_rows + slots * half_rows

    barrier = pltpu.get_barrier_semaphore()
    pl.semaphore_signal(barrier, inc=1, device_id=(part, 1 - feat), device_id_type=MESH)

    def greet(step, carry):
        peer = lax.rem(part + step, count)
        pl.semaphore_signal(barrier, inc=1, device_id=(peer, feat), device_id_type=MESH)
        return carry

    lax.fori_loop(1, count, greet, 0)

    columns = pl.ds(pl.multiple_of(feat * width, width), width)
    own_weight = weight_ref[pl.ds(pl.multiple_of(feat * depth, 16), depth), columns]
    other_weight = weight_ref[pl.ds(pl.multiple_of((1 - feat) * depth, 16), depth), columns]
    total_ref[...] = jnp.dot(features_ref[...], own_weight, preferred_element_type=jnp.float32)
    index_ref[...] = jnp.transpose(send_ref[...])

    hub_row = hub_ref[...]
    hub_col = jnp.transpose(jnp.broadcast_to(hub_row, (8, hub_total)))[:, :1]
    owner_row = hub_row // vertex_rows
    owner_col = hub_col // vertex_rows
    same = owner_row == owner_col
    first = lax.broadcasted_iota(jnp.int32, (hub_total, hub_total), 0)
    second = lax.broadcasted_iota(jnp.int32, (hub_total, hub_total), 1)
    rank_row = jnp.sum(jnp.where(same & (first < second), 1.0, 0.0), 0, keepdims=True)
    rank_col = jnp.sum(jnp.where(same & (second < first), 1.0, 0.0), 1, keepdims=True)
    rank_row = rank_row.astype(jnp.int32)
    rank_col = rank_col.astype(jnp.int32)
    local_col = jnp.clip(hub_col - part * vertex_rows, 0, vertex_rows - 1)
    ranks = lax.broadcasted_iota(jnp.int32, (HUB_MOST, hub_total), 0)
    selector = ((rank_row == ranks) & (owner_row == part)).astype(jnp.float32).astype(jnp.bfloat16)

    pl.semaphore_wait(barrier, count)

    exchange = pltpu.make_async_remote_copy(
        src_ref=features_ref, dst_ref=other_ref,
        send_sem=feature_sems.at[0], recv_sem=feature_sems.at[1],
        device_id=(part, 1 - feat), device_id_type=MESH,
    )
    exchange.start()
    exchange.wait_recv()
    group_rows = vertex_rows // GROUPS
    for group in range(GROUPS):
        rows = pl.ds(group * group_rows, group_rows)
        projected = total_ref[rows, :] + jnp.dot(
            other_ref[rows, :], other_weight, preferred_element_type=jnp.float32
        )
        projected = projected.astype(jnp.bfloat16)
        extended_ref[rows, :] = projected
        table_ref[:, group * width : (group + 1) * width] = projected

    candidates = picked_rows(local_col, table_ref, GROUPS)
    own_hubs = jnp.dot(selector, candidates, preferred_element_type=jnp.float32)
    own_hubs = own_hubs.astype(jnp.bfloat16)
    own_hubs_ref[...] = own_hubs
    hubs_ref[pl.ds(pl.multiple_of(part * HUB_MOST, 16), HUB_MOST), :] = own_hubs

    def hub_copy(step, source):
        return pltpu.make_async_remote_copy(
            src_ref=own_hubs_ref,
            dst_ref=hubs_ref.at[pl.ds(pl.multiple_of(source * HUB_MOST, 16), HUB_MOST), :],
            send_sem=hub_send_sems.at[step], recv_sem=hub_receive_sems.at[source],
            device_id=(lax.rem(part + step, count), feat), device_id_type=MESH,
        )

    def send_hubs(step, carry):
        hub_copy(step, part).start()
        return carry

    lax.fori_loop(1, count, send_hubs, 0)

    def halo_copy(slot):
        rows = pl.ds(vertex_rows + slot * half_rows, half_rows)
        return pltpu.make_async_remote_copy(
            src_ref=packed_ref.at[slot], dst_ref=extended_ref.at[rows, :],
            send_sem=send_sems.at[slot], recv_sem=receive_sems.at[slot],
            device_id=(lax.rem(part + offsets[slot] + count, count), feat), device_id_type=MESH,
        )

    chunk = math.gcd(half_rows, 512)
    order = sorted(range(slots), key=lambda slot: (abs(offsets[slot]) % 2 == 0, -abs(offsets[slot])))
    for slot in order:
        target = part + offsets[slot]
        present = (target >= 0) & (target < count)

        @pl.when(present)
        def _():
            for start in range(0, half_rows, chunk):
                index = index_ref[start : start + chunk, slot : slot + 1]
                packed_ref[slot, start : start + chunk, :] = picked_rows(index, table_ref, GROUPS)
            halo_copy(slot).start()

        source = part - offsets[slot]

        @pl.when((source < 0) | (source >= count))
        def _():
            rows = pl.ds(vertex_rows + slot * half_rows, half_rows)
            extended_ref[rows, :] = jnp.zeros((half_rows, width), jnp.bfloat16)

    def take_hubs(step, carry):
        hub_copy(step, lax.rem(part - step + count, count)).wait_recv()
        hub_copy(step, part).wait_send()
        return carry

    lax.fori_loop(1, count, take_hubs, 0)
    place = owner_col * HUB_MOST + rank_col
    extended_ref[halo_end : halo_end + hub_total, :] = picked_rows(place, hubs_ref, 1)
    exchange.wait_send()
    for slot in order:
        source = part - offsets[slot]
        target = part + offsets[slot]

        @pl.when((source >= 0) & (source < count))
        def _():
            halo_copy(slot).wait_recv()

        @pl.when((target >= 0) & (target < count))
        def _():
            halo_copy(slot).wait_send()


def tiles_kernel(
    rows_ref, cols_ref, count_ref, values_ref, extended_ref, bias_ref, out_ref, total_ref
):
    slots, edge, _ = values_ref.shape
    width = out_ref.shape[1]
    spare = out_ref.shape[0] // edge
    live = count_ref[0]
    total_ref[...] = jnp.zeros_like(total_ref)
    together = math.gcd(slots, 4)

    def step(number, carry):
        products, places = [], []
        for inner in range(together):
            slot = number * together + inner
            block = pl.ds(pl.multiple_of(cols_ref[slot] * edge, edge), edge)
            places.append(jnp.where(slot < live, rows_ref[slot], spare))
            products.append(
                jnp.dot(values_ref[slot], extended_ref[block, :], preferred_element_type=jnp.float32)
            )
        for place, product in zip(places, products):
            total_ref[pl.ds(pl.multiple_of(place * edge, edge), edge), :] += product
        return carry

    lax.fori_loop(0, (live + together - 1) // together, step, 0)
    summed = total_ref[: out_ref.shape[0], :] + bias_ref[...]
    out_ref[...] = jnp.maximum(summed, 0.0).astype(jnp.bfloat16)


def local(
    features, weight, out_bias, tile_values, tile_rows, tile_cols, tile_count, send_rows, hub_ids
):
    width = out_bias.shape[0]
    vertex_rows, depth = features.shape
    count = lax.axis_size("dom")
    _, slots, half_rows = send_rows.shape
    hub_total = hub_ids.shape[0]
    edge = tile_values.shape[1]
    vmem = pl.BlockSpec(memory_space=pltpu.VMEM)
    smem = pl.BlockSpec(memory_space=pltpu.SMEM)
    extended_rows = vertex_rows + slots * half_rows + hub_total
    extended = pl.pallas_call(
        functools.partial(exchange_kernel, count),
        out_shape=jax.ShapeDtypeStruct((extended_rows, width), jnp.bfloat16),
        in_specs=[vmem] * 4,
        out_specs=vmem,
        scratch_shapes=[
            pltpu.VMEM((vertex_rows, depth), jnp.bfloat16),
            pltpu.VMEM((vertex_rows, width), jnp.float32),
            pltpu.VMEM((vertex_rows // GROUPS, GROUPS * width), jnp.bfloat16),
            pltpu.VMEM((half_rows, slots), jnp.int32),
            pltpu.VMEM((slots, half_rows, width), jnp.bfloat16),
            pltpu.VMEM((HUB_MOST, width), jnp.bfloat16),
            pltpu.VMEM((count * HUB_MOST, width), jnp.bfloat16),
            pltpu.SemaphoreType.DMA((2,)),
            pltpu.SemaphoreType.DMA((slots,)),
            pltpu.SemaphoreType.DMA((slots,)),
            pltpu.SemaphoreType.DMA((count,)),
            pltpu.SemaphoreType.DMA((count,)),
        ],
        compiler_params=pltpu.CompilerParams(
            collective_id=0, has_side_effects=True, vmem_limit_bytes=32 << 20
        ),
    )(features, weight, send_rows[0], hub_ids[None, :])
    return pl.pallas_call(
        tiles_kernel,
        out_shape=jax.ShapeDtypeStruct((vertex_rows, width), jnp.bfloat16),
        in_specs=[smem] * 3 + [vmem] * 3,
        out_specs=vmem,
        scratch_shapes=[pltpu.VMEM((vertex_rows + edge, width), jnp.float32)],
        compiler_params=pltpu.CompilerParams(vmem_limit_bytes=24 << 20),
    )(tile_rows, tile_cols, tile_count, tile_values, extended, out_bias[None, :])


def solution(mesh):
    in_specs = (
        P("dom", "feat"),
        P(),
        P("feat"),
        P("dom", None, None),
        P("dom"),
        P("dom"),
        P("dom"),
        P("dom", None, None),
        P(),
    )
    out_specs = P("dom", "feat")

    def program(features, weight, out_bias, *rest):
        whole_lanes = out_bias.shape[0] % (LANES * mesh.shape["feat"]) == 0
        body = local if mesh.shape["feat"] == 2 and whole_lanes else local_any
        return jax.shard_map(
            body, mesh=mesh, in_specs=in_specs, out_specs=out_specs, check_vma=False
        )(features, weight, out_bias, *rest)

    return program
```

```python
import functools
import math

import jax
import jax.numpy as jnp
from jax import lax
from jax.experimental import pallas as pl
from jax.experimental.pallas import tpu as pltpu
from jax.sharding import PartitionSpec as P

REACH = 4
HUB_MOST = 48


def passed_along(value, axis, steps):
    count = lax.axis_size(axis)
    initial, last = (max(0, -steps), min(count, count - steps))
    return lax.ppermute(value, axis, [(source, source + steps) for source in range(initial, last)])


def local_any(
    features, weight, out_bias, tile_values, tile_rows, tile_cols, tile_count, send_rows, hub_ids
):
    column_count = out_bias.shape[0]
    vertex_rows = features.shape[0]
    part_index = lax.axis_index("dom")
    feat_index = lax.axis_index("feat")
    weight_cols = lax.dynamic_slice_in_dim(weight, feat_index * column_count, column_count, 1)
    summed = jnp.dot(
        lax.all_gather(features, "feat", axis=1, tiled=True),
        weight_cols,
        preferred_element_type=jnp.float32,
    )
    projected = summed.astype(jnp.bfloat16)
    half_rows = send_rows.shape[2]
    slot_total = send_rows.shape[1]
    offsets = list(range(-REACH, 0)) + list(range(1, REACH + 1))
    packed_all = projected[send_rows[0].reshape(slot_total * half_rows)].reshape(
        slot_total, half_rows, column_count
    )
    received = []
    for slot_index, offset_value in enumerate(offsets):
        received.append(passed_along(packed_all[slot_index], "dom", offset_value))
    halo_block = jnp.concatenate(received, 0)
    owners = hub_ids // vertex_rows
    mine = owners == part_index
    local_index = jnp.clip(hub_ids - part_index * vertex_rows, 0, vertex_rows - 1)
    candidates = projected[local_index]
    hub_total = hub_ids.shape[0]
    positions = jnp.arange(hub_total, dtype=jnp.int32)
    earlier = (owners[:, None] == owners[None, :]) & (positions[:, None] > positions[None, :])
    ranks = jnp.sum(earlier.astype(jnp.int32), 1)
    selector = (
        mine[:, None] & (ranks[:, None] == jnp.arange(HUB_MOST, dtype=jnp.int32)[None, :])
    ).astype(jnp.bfloat16)
    slot_rows = lax.dot_general(
        selector, candidates, (((0,), (0,)), ((), ())), preferred_element_type=jnp.float32
    ).astype(jnp.bfloat16)
    gathered = lax.all_gather(slot_rows, "dom", axis=0, tiled=True)
    hub_block = gathered[owners * HUB_MOST + ranks]
    extended = jnp.concatenate([projected, halo_block, hub_block], 0)
    block_edge = tile_values.shape[1]
    blocks = extended.reshape(extended.shape[0] // block_edge, block_edge, column_count)
    products = jnp.einsum(
        "tij,tjc->tic", tile_values, blocks[tile_cols], preferred_element_type=jnp.float32
    )
    live_mask = jnp.arange(tile_values.shape[0], dtype=jnp.int32) < tile_count[0]
    block_count = vertex_rows // block_edge
    assignment = (
        (tile_rows[None, :] == jnp.arange(block_count, dtype=jnp.int32)[:, None])
        & live_mask[None, :]
    ).astype(jnp.float32)
    aggregate = jnp.einsum("rt,tic->ric", assignment, products, precision=lax.Precision.HIGHEST)
    activated = jnp.maximum(aggregate + out_bias[None, None, :], 0.0).astype(jnp.bfloat16)
    return activated.reshape(vertex_rows, column_count)

LANES = 128
GROUPS = 4
PLANE = 4
MESH = pl.DeviceIdType.MESH


def picked_rows(index, table_ref, groups):
    depth = table_ref.shape[0]
    group = index // depth
    within = index - group * depth
    positions = lax.broadcasted_iota(jnp.int32, (index.shape[0], depth), 1)
    chosen = (positions == within).astype(jnp.float32).astype(jnp.bfloat16)
    every = jnp.dot(chosen, table_ref[...], preferred_element_type=jnp.float32)
    width = table_ref.shape[1] // groups
    result = every[:, :width]
    for number in range(1, groups):
        part = every[:, number * width : (number + 1) * width]
        result = jnp.where(group == number, part, result)
    return result.astype(jnp.bfloat16)


def over_rows(left, right):
    dims = (((0,), (0,)), ((), ()))
    return lax.dot_general(left, right, dims, preferred_element_type=jnp.float32)


def exchange_kernel(
    count, features_ref, weight_ref, send_ref, hub_ref, extended_ref,
    other_ref, total_ref, table_ref, index_ref, packed_ref, own_hubs_ref, hubs_ref,
    feature_sems, send_sems, receive_sems, hub_send_sems, hub_receive_sems,
):
    part = lax.axis_index("dom")
    feat = lax.axis_index("feat")
    depth, vertex_rows = features_ref.shape
    width = extended_ref.shape[1]
    lines = count // PLANE
    line = part // PLANE
    group_rows = vertex_rows // GROUPS
    slots, half_rows = send_ref.shape
    offsets = list(range(-REACH, 0)) + list(range(1, REACH + 1))
    hub_total = hub_ref.shape[1]
    halo_end = vertex_rows + slots * half_rows

    barrier = pltpu.get_barrier_semaphore()
    pl.semaphore_signal(barrier, inc=1, device_id=(part, 1 - feat), device_id_type=MESH)

    def greet(step, carry):
        peer = lax.rem(part + step * PLANE, count)
        pl.semaphore_signal(barrier, inc=1, device_id=(peer, feat), device_id_type=MESH)
        return carry

    lax.fori_loop(1, lines, greet, 0)
    greeted = lines
    for offset in offsets:
        if abs(offset) % PLANE != 0:
            target = part + offset
            inside = (target >= 0) & (target < count)
            greeted = greeted + inside.astype(jnp.int32)

            @pl.when(inside)
            def _():
                pl.semaphore_signal(
                    barrier, inc=1, device_id=(target, feat), device_id_type=MESH
                )

    columns = pl.ds(pl.multiple_of(feat * width, width), width)
    own_weight = weight_ref[pl.ds(pl.multiple_of(feat * depth, 16), depth), columns]
    other_weight = weight_ref[pl.ds(pl.multiple_of((1 - feat) * depth, 16), depth), columns]
    total_ref[...] = over_rows(own_weight, features_ref[...])
    index_ref[...] = jnp.transpose(send_ref[...])

    hub_row = hub_ref[...]
    hub_col = jnp.transpose(jnp.broadcast_to(hub_row, (8, hub_total)))[:, :1]
    owner_row = hub_row // vertex_rows
    owner_col = hub_col // vertex_rows
    same = owner_row == owner_col
    first = lax.broadcasted_iota(jnp.int32, (hub_total, hub_total), 0)
    second = lax.broadcasted_iota(jnp.int32, (hub_total, hub_total), 1)
    rank_row = jnp.sum(jnp.where(same & (first < second), 1.0, 0.0), 0, keepdims=True)
    rank_col = jnp.sum(jnp.where(same & (second < first), 1.0, 0.0), 1, keepdims=True)
    rank_row = rank_row.astype(jnp.int32)
    rank_col = rank_col.astype(jnp.int32)
    local_col = jnp.clip(hub_col - part * vertex_rows, 0, vertex_rows - 1)
    ranks = lax.broadcasted_iota(jnp.int32, (HUB_MOST, hub_total), 0)
    selector = ((rank_row == ranks) & (owner_row == part)).astype(jnp.float32).astype(jnp.bfloat16)

    pl.semaphore_wait(barrier, greeted)

    exchanges = []
    for group in range(GROUPS):
        columns = pl.ds(group * group_rows, group_rows)
        exchanges.append(
            pltpu.make_async_remote_copy(
                src_ref=features_ref.at[:, columns], dst_ref=other_ref.at[:, columns],
                send_sem=feature_sems.at[0, group], recv_sem=feature_sems.at[1, group],
                device_id=(part, 1 - feat), device_id_type=MESH,
            )
        )
        exchanges[group].start()
    for group in range(GROUPS):
        rows = pl.ds(group * group_rows, group_rows)
        exchanges[group].wait_recv()
        projected = total_ref[:, rows] + over_rows(other_weight, other_ref[:, rows])
        projected = jnp.transpose(projected).astype(jnp.bfloat16)
        extended_ref[rows, :] = projected
        table_ref[:, group * width : (group + 1) * width] = projected

    candidates = picked_rows(local_col, table_ref, GROUPS)
    own_hubs = jnp.dot(selector, candidates, preferred_element_type=jnp.float32)
    own_hubs = own_hubs.astype(jnp.bfloat16)
    own_hubs_ref[...] = own_hubs
    hubs_ref[pl.ds(pl.multiple_of(part * HUB_MOST, 16), HUB_MOST), :] = own_hubs

    def hub_copy(number, first, blocks, target, source_ref=None):
        rows = pl.ds(pl.multiple_of(first * HUB_MOST, 16), blocks * HUB_MOST)
        return pltpu.make_async_remote_copy(
            src_ref=hubs_ref.at[rows, :] if source_ref is None else source_ref,
            dst_ref=hubs_ref.at[rows, :],
            send_sem=hub_send_sems.at[number], recv_sem=hub_receive_sems.at[number],
            device_id=(target, feat), device_id_type=MESH,
        )

    side = lax.rem(part, 2)
    across = part + 1 - 2 * side
    pair = part - side
    pair_side = lax.rem(part // 2, 2)
    far = part + 2 - 4 * pair_side
    far_pair = pair + 2 - 4 * pair_side
    plane = line * PLANE

    def line_copy(step, first):
        return hub_copy(1 + step, first, PLANE, lax.rem(part + step * PLANE, count))

    hub_copy(0, part, 1, across, own_hubs_ref).start()

    def halo_copy(slot):
        rows = pl.ds(vertex_rows + slot * half_rows, half_rows)
        return pltpu.make_async_remote_copy(
            src_ref=packed_ref.at[slot], dst_ref=extended_ref.at[rows, :],
            send_sem=send_sems.at[slot], recv_sem=receive_sems.at[slot],
            device_id=(lax.rem(part + offsets[slot] + count, count), feat), device_id_type=MESH,
        )

    chunk = math.gcd(half_rows, 512)
    order = sorted(range(slots), key=lambda slot: (abs(offsets[slot]) % 2 == 0, -abs(offsets[slot])))
    for number, slot in enumerate(order):
        if number == 2:
            hub_copy(0, across, 1, across, own_hubs_ref).wait_recv()
            hub_copy(1, pair, 2, far).start()
        if number == 5:
            hub_copy(1, far_pair, 2, far).wait_recv()
            for step in range(1, lines):
                line_copy(step, plane).start()
        target = part + offsets[slot]
        present = (target >= 0) & (target < count)

        @pl.when(present)
        def _():
            for start in range(0, half_rows, chunk):
                index = index_ref[start : start + chunk, slot : slot + 1]
                packed_ref[slot, start : start + chunk, :] = picked_rows(index, table_ref, GROUPS)
            halo_copy(slot).start()

        source = part - offsets[slot]

        @pl.when((source < 0) | (source >= count))
        def _():
            rows = pl.ds(vertex_rows + slot * half_rows, half_rows)
            extended_ref[rows, :] = jnp.zeros((half_rows, width), jnp.bfloat16)

    for step in range(1, lines):
        line_copy(step, lax.rem(line - step + lines, lines) * PLANE).wait_recv()
    place = owner_col * HUB_MOST + rank_col
    extended_ref[halo_end : halo_end + hub_total, :] = picked_rows(place, hubs_ref, 1)
    for exchange in exchanges:
        exchange.wait_send()
    hub_copy(0, part, 1, across, own_hubs_ref).wait_send()
    hub_copy(1, pair, 2, far).wait_send()
    for step in range(1, lines):
        line_copy(step, plane).wait_send()
    for slot in order:
        source = part - offsets[slot]
        target = part + offsets[slot]

        @pl.when((source >= 0) & (source < count))
        def _():
            halo_copy(slot).wait_recv()

        @pl.when((target >= 0) & (target < count))
        def _():
            halo_copy(slot).wait_send()


def tiles_kernel(
    rows_ref, cols_ref, count_ref, values_ref, extended_ref, bias_ref, out_ref, total_ref
):
    slots, edge, _ = values_ref.shape
    width = out_ref.shape[1]
    spare = out_ref.shape[0] // edge
    live = count_ref[0]
    total_ref[...] = jnp.zeros_like(total_ref)
    together = math.gcd(slots, 12)

    def step(number, carry):
        products, places = [], []
        for inner in range(together):
            slot = number * together + inner
            block = pl.ds(pl.multiple_of(cols_ref[slot] * edge, edge), edge)
            places.append(jnp.where(slot < live, rows_ref[slot], spare))
            products.append(
                jnp.dot(values_ref[slot], extended_ref[block, :], preferred_element_type=jnp.float32)
            )
        for place, product in zip(places, products):
            total_ref[pl.ds(pl.multiple_of(place * edge, edge), edge), :] += product
        return carry

    lax.fori_loop(0, (live + together - 1) // together, step, 0)
    summed = total_ref[: out_ref.shape[0], :] + bias_ref[...]
    out_ref[...] = jnp.maximum(summed, 0.0).astype(jnp.bfloat16)


def local(
    features, weight, out_bias, tile_values, tile_rows, tile_cols, tile_count, send_rows, hub_ids
):
    width = out_bias.shape[0]
    vertex_rows, depth = features.shape
    count = lax.axis_size("dom")
    _, slots, half_rows = send_rows.shape
    hub_total = hub_ids.shape[0]
    edge = tile_values.shape[1]
    vmem = pl.BlockSpec(memory_space=pltpu.VMEM)
    smem = pl.BlockSpec(memory_space=pltpu.SMEM)
    extended_rows = vertex_rows + slots * half_rows + hub_total
    extended = pl.pallas_call(
        functools.partial(exchange_kernel, count),
        out_shape=jax.ShapeDtypeStruct((extended_rows, width), jnp.bfloat16),
        in_specs=[vmem] * 4,
        out_specs=vmem,
        scratch_shapes=[
            pltpu.VMEM((depth, vertex_rows), jnp.bfloat16),
            pltpu.VMEM((width, vertex_rows), jnp.float32),
            pltpu.VMEM((vertex_rows // GROUPS, GROUPS * width), jnp.bfloat16),
            pltpu.VMEM((half_rows, slots), jnp.int32),
            pltpu.VMEM((slots, half_rows, width), jnp.bfloat16),
            pltpu.VMEM((HUB_MOST, width), jnp.bfloat16),
            pltpu.VMEM((count * HUB_MOST, width), jnp.bfloat16),
            pltpu.SemaphoreType.DMA((2, GROUPS)),
            pltpu.SemaphoreType.DMA((slots,)),
            pltpu.SemaphoreType.DMA((slots,)),
            pltpu.SemaphoreType.DMA((count // PLANE + 1,)),
            pltpu.SemaphoreType.DMA((count // PLANE + 1,)),
        ],
        compiler_params=pltpu.CompilerParams(
            collective_id=0, has_side_effects=True, vmem_limit_bytes=32 << 20
        ),
    )(jnp.transpose(features), weight, send_rows[0], hub_ids[None, :])
    return pl.pallas_call(
        tiles_kernel,
        out_shape=jax.ShapeDtypeStruct((vertex_rows, width), jnp.bfloat16),
        in_specs=[smem] * 3 + [vmem] * 3,
        out_specs=vmem,
        scratch_shapes=[pltpu.VMEM((vertex_rows + edge, width), jnp.float32)],
        compiler_params=pltpu.CompilerParams(vmem_limit_bytes=24 << 20),
    )(tile_rows, tile_cols, tile_count, tile_values, extended, out_bias[None, :])


def solution(mesh):
    in_specs = (
        P("dom", "feat"),
        P(),
        P("feat"),
        P("dom", None, None),
        P("dom"),
        P("dom"),
        P("dom"),
        P("dom", None, None),
        P(),
    )
    out_specs = P("dom", "feat")

    def program(features, weight, out_bias, *rest):
        whole_lanes = out_bias.shape[0] % (LANES * mesh.shape["feat"]) == 0
        fits = mesh.shape["feat"] == 2 and mesh.shape["dom"] % PLANE == 0
        body = local if fits and whole_lanes else local_any
        return jax.shard_map(
            body, mesh=mesh, in_specs=in_specs, out_specs=out_specs, check_vma=False
        )(features, weight, out_bias, *rest)

    return program
```

```python
import functools
import math

import jax
import jax.numpy as jnp
from jax import lax
from jax.experimental import pallas as pl
from jax.experimental.pallas import tpu as pltpu
from jax.sharding import PartitionSpec as P

REACH = 4
HUB_MOST = 48


def passed_along(value, axis, steps):
    count = lax.axis_size(axis)
    initial, last = (max(0, -steps), min(count, count - steps))
    return lax.ppermute(value, axis, [(source, source + steps) for source in range(initial, last)])


def local_any(
    features, weight, out_bias, tile_values, tile_rows, tile_cols, tile_count, send_rows, hub_ids
):
    column_count = out_bias.shape[0]
    vertex_rows = features.shape[0]
    part_index = lax.axis_index("dom")
    feat_index = lax.axis_index("feat")
    weight_cols = lax.dynamic_slice_in_dim(weight, feat_index * column_count, column_count, 1)
    summed = jnp.dot(
        lax.all_gather(features, "feat", axis=1, tiled=True),
        weight_cols,
        preferred_element_type=jnp.float32,
    )
    projected = summed.astype(jnp.bfloat16)
    half_rows = send_rows.shape[2]
    slot_total = send_rows.shape[1]
    offsets = list(range(-REACH, 0)) + list(range(1, REACH + 1))
    packed_all = projected[send_rows[0].reshape(slot_total * half_rows)].reshape(
        slot_total, half_rows, column_count
    )
    received = []
    for slot_index, offset_value in enumerate(offsets):
        received.append(passed_along(packed_all[slot_index], "dom", offset_value))
    halo_block = jnp.concatenate(received, 0)
    owners = hub_ids // vertex_rows
    mine = owners == part_index
    local_index = jnp.clip(hub_ids - part_index * vertex_rows, 0, vertex_rows - 1)
    candidates = projected[local_index]
    hub_total = hub_ids.shape[0]
    positions = jnp.arange(hub_total, dtype=jnp.int32)
    earlier = (owners[:, None] == owners[None, :]) & (positions[:, None] > positions[None, :])
    ranks = jnp.sum(earlier.astype(jnp.int32), 1)
    selector = (
        mine[:, None] & (ranks[:, None] == jnp.arange(HUB_MOST, dtype=jnp.int32)[None, :])
    ).astype(jnp.bfloat16)
    slot_rows = lax.dot_general(
        selector, candidates, (((0,), (0,)), ((), ())), preferred_element_type=jnp.float32
    ).astype(jnp.bfloat16)
    gathered = lax.all_gather(slot_rows, "dom", axis=0, tiled=True)
    hub_block = gathered[owners * HUB_MOST + ranks]
    extended = jnp.concatenate([projected, halo_block, hub_block], 0)
    block_edge = tile_values.shape[1]
    blocks = extended.reshape(extended.shape[0] // block_edge, block_edge, column_count)
    products = jnp.einsum(
        "tij,tjc->tic", tile_values, blocks[tile_cols], preferred_element_type=jnp.float32
    )
    live_mask = jnp.arange(tile_values.shape[0], dtype=jnp.int32) < tile_count[0]
    block_count = vertex_rows // block_edge
    assignment = (
        (tile_rows[None, :] == jnp.arange(block_count, dtype=jnp.int32)[:, None])
        & live_mask[None, :]
    ).astype(jnp.float32)
    aggregate = jnp.einsum("rt,tic->ric", assignment, products, precision=lax.Precision.HIGHEST)
    activated = jnp.maximum(aggregate + out_bias[None, None, :], 0.0).astype(jnp.bfloat16)
    return activated.reshape(vertex_rows, column_count)

LANES = 128
GROUPS = 4
PLANE = 4
PIECES = 2
MESH = pl.DeviceIdType.MESH


def picked_rows(index, table_ref, groups):
    depth = table_ref.shape[0]
    group = index // depth
    within = index - group * depth
    positions = lax.broadcasted_iota(jnp.int32, (index.shape[0], depth), 1)
    chosen = (positions == within).astype(jnp.float32).astype(jnp.bfloat16)
    every = jnp.dot(chosen, table_ref[...], preferred_element_type=jnp.float32)
    width = table_ref.shape[1] // groups
    result = every[:, :width]
    for number in range(1, groups):
        part = every[:, number * width : (number + 1) * width]
        result = jnp.where(group == number, part, result)
    return result.astype(jnp.bfloat16)


def over_rows(left, right):
    dims = (((0,), (0,)), ((), ()))
    return lax.dot_general(left, right, dims, preferred_element_type=jnp.float32)


def exchange_kernel(
    count, features_hbm, weight_hbm, send_hbm, hub_ref, extended_ref,
    features_ref, weight_ref, send_ref, load_sems,
    other_ref, total_ref, table_ref, index_ref, packed_ref, own_hubs_ref, hubs_ref,
    feature_sems, send_sems, receive_sems, hub_send_sems, hub_receive_sems,
):
    part = lax.axis_index("dom")
    feat = lax.axis_index("feat")
    depth, vertex_rows = features_ref.shape
    width = extended_ref.shape[1]
    loads = []
    for number, (source, target) in enumerate(
        ((weight_hbm, weight_ref), (features_hbm, features_ref), (send_hbm, send_ref))
    ):
        loads.append(pltpu.make_async_copy(source, target, load_sems.at[number]))
        loads[number].start()
    lines = count // PLANE
    line = part // PLANE
    group_rows = vertex_rows // GROUPS
    slots, half_rows = send_ref.shape
    chunk = half_rows // PIECES
    offsets = list(range(-REACH, 0)) + list(range(1, REACH + 1))
    hub_total = hub_ref.shape[1]
    halo_end = vertex_rows + slots * half_rows

    barrier = pltpu.get_barrier_semaphore()
    pl.semaphore_signal(barrier, inc=1, device_id=(part, 1 - feat), device_id_type=MESH)

    def greet(step, carry):
        peer = lax.rem(part + step * PLANE, count)
        pl.semaphore_signal(barrier, inc=1, device_id=(peer, feat), device_id_type=MESH)
        return carry

    lax.fori_loop(1, lines, greet, 0)
    greeted = lines
    for offset in offsets:
        if abs(offset) % PLANE != 0:
            target = part + offset
            inside = (target >= 0) & (target < count)
            greeted = greeted + inside.astype(jnp.int32)

            @pl.when(inside)
            def _():
                pl.semaphore_signal(
                    barrier, inc=1, device_id=(target, feat), device_id_type=MESH
                )

    hub_row = hub_ref[...]
    hub_col = jnp.transpose(jnp.broadcast_to(hub_row, (8, hub_total)))[:, :1]
    owner_row = hub_row // vertex_rows
    owner_col = hub_col // vertex_rows
    same = owner_row == owner_col
    first = lax.broadcasted_iota(jnp.int32, (hub_total, hub_total), 0)
    second = lax.broadcasted_iota(jnp.int32, (hub_total, hub_total), 1)
    rank_row = jnp.sum(jnp.where(same & (first < second), 1.0, 0.0), 0, keepdims=True)
    rank_col = jnp.sum(jnp.where(same & (second < first), 1.0, 0.0), 1, keepdims=True)
    rank_row = rank_row.astype(jnp.int32)
    rank_col = rank_col.astype(jnp.int32)
    ranks = lax.broadcasted_iota(jnp.int32, (HUB_MOST, hub_total), 0)
    chosen = (rank_row == ranks) & (owner_row == part)
    local_row = (hub_row - part * vertex_rows).astype(jnp.float32)
    own_index = jnp.sum(jnp.where(chosen, local_row, 0.0), 1, keepdims=True).astype(jnp.int32)
    loads[0].wait()
    loads[1].wait()
    columns = pl.ds(pl.multiple_of(feat * width, width), width)
    own_weight = weight_ref[pl.ds(pl.multiple_of(feat * depth, 16), depth), columns]
    other_weight = weight_ref[pl.ds(pl.multiple_of((1 - feat) * depth, 16), depth), columns]
    total_ref[...] = over_rows(own_weight, features_ref[...])
    loads[2].wait()
    index_ref[...] = jnp.transpose(send_ref[...])

    pl.semaphore_wait(barrier, greeted)

    exchanges = []
    for group in range(GROUPS):
        columns = pl.ds(group * group_rows, group_rows)
        exchanges.append(
            pltpu.make_async_remote_copy(
                src_ref=features_hbm.at[:, columns], dst_ref=other_ref.at[:, columns],
                send_sem=feature_sems.at[0, group], recv_sem=feature_sems.at[1, group],
                device_id=(part, 1 - feat), device_id_type=MESH,
            )
        )
        exchanges[group].start()
    for group in range(GROUPS):
        rows = pl.ds(group * group_rows, group_rows)
        exchanges[group].wait_recv()
        projected = total_ref[:, rows] + over_rows(other_weight, other_ref[:, rows])
        projected = jnp.transpose(projected).astype(jnp.bfloat16)
        extended_ref[rows, :] = projected
        table_ref[:, group * width : (group + 1) * width] = projected

    own_hubs = picked_rows(own_index, table_ref, GROUPS)
    own_hubs_ref[...] = own_hubs
    hubs_ref[pl.ds(pl.multiple_of(part * HUB_MOST, 16), HUB_MOST), :] = own_hubs

    def hub_copy(number, first, blocks, target, source_ref=None):
        rows = pl.ds(pl.multiple_of(first * HUB_MOST, 16), blocks * HUB_MOST)
        return pltpu.make_async_remote_copy(
            src_ref=hubs_ref.at[rows, :] if source_ref is None else source_ref,
            dst_ref=hubs_ref.at[rows, :],
            send_sem=hub_send_sems.at[number], recv_sem=hub_receive_sems.at[number],
            device_id=(target, feat), device_id_type=MESH,
        )

    side = lax.rem(part, 2)
    across = part + 1 - 2 * side
    pair = part - side
    pair_side = lax.rem(part // 2, 2)
    far = part + 2 - 4 * pair_side
    far_pair = pair + 2 - 4 * pair_side
    plane = line * PLANE

    def line_copy(step, first):
        return hub_copy(1 + step, first, PLANE, lax.rem(part + step * PLANE, count))

    hub_copy(0, part, 1, across, own_hubs_ref).start()

    def halo_copy(slot, piece):
        rows = pl.ds(vertex_rows + slot * half_rows + piece * chunk, chunk)
        return pltpu.make_async_remote_copy(
            src_ref=packed_ref.at[slot, piece * chunk : (piece + 1) * chunk, :], dst_ref=extended_ref.at[rows, :],
            send_sem=send_sems.at[slot, piece], recv_sem=receive_sems.at[slot, piece],
            device_id=(lax.rem(part + offsets[slot] + count, count), feat), device_id_type=MESH,
        )

    order = sorted(range(slots), key=lambda slot: (abs(offsets[slot]) % 2 == 0, -abs(offsets[slot])))
    for number, slot in enumerate(order):
        if number == 2:
            hub_copy(0, across, 1, across, own_hubs_ref).wait_recv()
            hub_copy(1, pair, 2, far).start()
        if number == 5:
            hub_copy(1, far_pair, 2, far).wait_recv()
            for step in range(1, lines):
                line_copy(step, plane).start()
        target = part + offsets[slot]
        present = (target >= 0) & (target < count)

        @pl.when(present)
        def _():
            for piece in range(PIECES):
                rows = pl.ds(piece * chunk, chunk)
                index = index_ref[rows, slot : slot + 1]
                packed_ref[slot, rows, :] = picked_rows(index, table_ref, GROUPS)
                halo_copy(slot, piece).start()

        source = part - offsets[slot]

        @pl.when((source < 0) | (source >= count))
        def _():
            rows = pl.ds(vertex_rows + slot * half_rows, half_rows)
            extended_ref[rows, :] = jnp.zeros((half_rows, width), jnp.bfloat16)

    for step in range(1, lines):
        line_copy(step, lax.rem(line - step + lines, lines) * PLANE).wait_recv()
    place = owner_col * HUB_MOST + rank_col
    extended_ref[halo_end : halo_end + hub_total, :] = picked_rows(place, hubs_ref, 1)
    for exchange in exchanges:
        exchange.wait_send()
    hub_copy(0, part, 1, across, own_hubs_ref).wait_send()
    hub_copy(1, pair, 2, far).wait_send()
    for step in range(1, lines):
        line_copy(step, plane).wait_send()
    for slot in order:
        source = part - offsets[slot]
        target = part + offsets[slot]

        @pl.when((source >= 0) & (source < count))
        def _():
            for piece in range(PIECES):
                halo_copy(slot, piece).wait_recv()

        @pl.when((target >= 0) & (target < count))
        def _():
            for piece in range(PIECES):
                halo_copy(slot, piece).wait_send()


def tiles_kernel(
    rows_ref, cols_ref, count_ref, values_ref, extended_ref, bias_ref, out_ref, total_ref
):
    slots, edge, _ = values_ref.shape
    width = out_ref.shape[1]
    spare = out_ref.shape[0] // edge
    live = count_ref[0]
    total_ref[...] = jnp.zeros_like(total_ref)
    together = math.gcd(slots, 12)

    def step(number, carry):
        products, places = [], []
        for inner in range(together):
            slot = number * together + inner
            block = pl.ds(pl.multiple_of(cols_ref[slot] * edge, edge), edge)
            places.append(jnp.where(slot < live, rows_ref[slot], spare))
            products.append(
                jnp.dot(values_ref[slot], extended_ref[block, :], preferred_element_type=jnp.float32)
            )
        for place, product in zip(places, products):
            total_ref[pl.ds(pl.multiple_of(place * edge, edge), edge), :] += product
        return carry

    lax.fori_loop(0, (live + together - 1) // together, step, 0)
    summed = total_ref[: out_ref.shape[0], :] + bias_ref[...]
    out_ref[...] = jnp.maximum(summed, 0.0).astype(jnp.bfloat16)


def local(
    features, weight, out_bias, tile_values, tile_rows, tile_cols, tile_count, send_rows, hub_ids
):
    width = out_bias.shape[0]
    vertex_rows, depth = features.shape
    count = lax.axis_size("dom")
    _, slots, half_rows = send_rows.shape
    hub_total = hub_ids.shape[0]
    edge = tile_values.shape[1]
    vmem = pl.BlockSpec(memory_space=pltpu.VMEM)
    smem = pl.BlockSpec(memory_space=pltpu.SMEM)
    extended_rows = vertex_rows + slots * half_rows + hub_total
    extended = pl.pallas_call(
        functools.partial(exchange_kernel, count),
        out_shape=jax.ShapeDtypeStruct((extended_rows, width), jnp.bfloat16),
        in_specs=[pl.BlockSpec(memory_space=pltpu.HBM)] * 3 + [vmem],
        out_specs=vmem,
        scratch_shapes=[
            pltpu.VMEM((depth, vertex_rows), jnp.bfloat16),
            pltpu.VMEM(weight.shape, jnp.bfloat16),
            pltpu.VMEM((slots, half_rows), jnp.int32),
            pltpu.SemaphoreType.DMA((3,)),
            pltpu.VMEM((depth, vertex_rows), jnp.bfloat16),
            pltpu.VMEM((width, vertex_rows), jnp.float32),
            pltpu.VMEM((vertex_rows // GROUPS, GROUPS * width), jnp.bfloat16),
            pltpu.VMEM((half_rows, slots), jnp.int32),
            pltpu.VMEM((slots, half_rows, width), jnp.bfloat16),
            pltpu.VMEM((HUB_MOST, width), jnp.bfloat16),
            pltpu.VMEM((count * HUB_MOST, width), jnp.bfloat16),
            pltpu.SemaphoreType.DMA((2, GROUPS)),
            pltpu.SemaphoreType.DMA((slots, PIECES)),
            pltpu.SemaphoreType.DMA((slots, PIECES)),
            pltpu.SemaphoreType.DMA((count // PLANE + 1,)),
            pltpu.SemaphoreType.DMA((count // PLANE + 1,)),
        ],
        compiler_params=pltpu.CompilerParams(
            collective_id=0, has_side_effects=True, vmem_limit_bytes=32 << 20
        ),
    )(jnp.transpose(features), weight, send_rows[0], hub_ids[None, :])
    return pl.pallas_call(
        tiles_kernel,
        out_shape=jax.ShapeDtypeStruct((vertex_rows, width), jnp.bfloat16),
        in_specs=[smem] * 3 + [vmem] * 3,
        out_specs=vmem,
        scratch_shapes=[pltpu.VMEM((vertex_rows + edge, width), jnp.float32)],
        compiler_params=pltpu.CompilerParams(vmem_limit_bytes=24 << 20),
    )(tile_rows, tile_cols, tile_count, tile_values, extended, out_bias[None, :])


def solution(mesh):
    in_specs = (
        P("dom", "feat"),
        P(),
        P("feat"),
        P("dom", None, None),
        P("dom"),
        P("dom"),
        P("dom"),
        P("dom", None, None),
        P(),
    )
    out_specs = P("dom", "feat")

    def program(features, weight, out_bias, *rest):
        whole_lanes = out_bias.shape[0] % (LANES * mesh.shape["feat"]) == 0
        fits = mesh.shape["feat"] == 2 and mesh.shape["dom"] % PLANE == 0
        body = local if fits and whole_lanes else local_any
        return jax.shard_map(
            body, mesh=mesh, in_specs=in_specs, out_specs=out_specs, check_vma=False
        )(features, weight, out_bias, *rest)

    return program
```
